32 devices in a mesh: gx: 32 (over z, y, x, core).
Axes of the slice: x: 2, y: 2, z: 4, core: 2. Of those that a mesh axis runs over, the one named last changes fastest.
Arguments:
- fine: bfloat16 [64, 8192, 128], P(None, 'gx'), may hold values from -6 to 6
- pattern: int32 [8, 8192], P(None, 'gx'), may hold values from 0 to 3
- stencil: bfloat16 [3, 128, 128], replicated, may hold values from -0.3125 to 0.3125
- restrict: bfloat16 [8, 4, 128, 128], replicated, may hold values from -0.5 to 0.5
- coarse_inv: bfloat16 [8, 128, 128], replicated, may hold values from -0.5 to 0.5
Outputs:
- smoothed: float32 [64, 8192, 128], P(None, 'gx')
The draws below stay inside these ranges and needn't reach their ends.
All inputs are finite; a program needn't handle non-finite values.
Results may differ from the reference program's by a relative error of at most 0.0046.
Values may be sent and summed in bfloat16 or wider, within the bound.
No kernel may reach another device: no remote copies, remote signals or barrier semaphores. Data moves between devices by JAX's collectives and lax.ppermute only.
A program may use at most 128 MiB of HBM per device.

```python
import jax
import jax.numpy as jnp
from jax import lax

WIDTH = 128
KINDS = 4
LEVELS = 8
BLK_DEV = 256
NVEC = 64
NB = 8192


def touch_ends(values, rng, least, high):
    place = [jax.random.randint(jax.random.fold_in(rng, axis), (), 0, length) for axis, length in enumerate(values.shape)]
    widest = values.shape.index(max(values.shape))
    next_to = place[:widest] + [(place[widest] + 1) % values.shape[widest]] + place[widest + 1:]
    return values.at[tuple(place)].set(least).at[tuple(next_to)].set(high)


def block_levels(key, shape, pieces, low, top_value):
    def one(axis_at, parts):
        steps = jax.random.uniform(jax.random.fold_in(jax.random.fold_in(key, 6), axis_at), (parts,), jnp.float32, low / len(pieces), top_value / len(pieces))
        return jnp.repeat(jnp.exp(steps), shape[axis_at] // parts).reshape((-1,) + (1,) * (len(shape) - axis_at - 1))

    factor_of = one(*pieces[0])
    for cut in pieces[1:]:
        factor_of = factor_of * one(*cut)
    return factor_of


def gaussian(rng, dims, scale, reach, cuts=(), held_as=jnp.bfloat16):
    values = jax.random.normal(rng, dims, jnp.float32) * scale
    if len(cuts) > 0:
        values = block_levels(rng, dims, cuts, -0.22, 0.18) * values
    return jnp.clip(values, min=-reach, max=reach).astype(held_as)


def setup_inputs(seed: int = 0) -> dict:
    key_list = jax.random.split(jax.random.key(seed), 6)
    fine = gaussian(key_list[0], (NVEC, NB, WIDTH), 1.0, 6.0, ((1, 32),))
    pattern = touch_ends(jax.random.randint(key_list[1], (LEVELS, NB), 0, KINDS), jax.random.fold_in(key_list[1], 1), 0, KINDS - 1).astype(jnp.int32)
    stencil = gaussian(key_list[2], (3, WIDTH, WIDTH), (3 * WIDTH) ** -0.5, 0.3125)
    restrict = gaussian(key_list[3], (LEVELS, KINDS, WIDTH, WIDTH), WIDTH ** -0.5, 0.5)
    coarse_inv = gaussian(key_list[4], (LEVELS, WIDTH, WIDTH), WIDTH ** -0.5, 0.5)
    return {"fine": fine, "pattern": pattern, "stencil": stencil, "restrict": restrict, "coarse_inv": coarse_inv}


EXACT = lax.Precision.HIGHEST


def one_vector(fine_vec, pattern, stencil, restrict, coarse_inv):
    all_blocks = fine_vec.shape[0]
    width = fine_vec.shape[1]
    earlier = jnp.roll(fine_vec, 1, axis=0)
    later = jnp.roll(fine_vec, -1, axis=0)
    result = jnp.dot(earlier, stencil[0], preferred_element_type=jnp.float32)
    result = result + jnp.dot(fine_vec, stencil[1], preferred_element_type=jnp.float32)
    result = result + jnp.dot(later, stencil[2], preferred_element_type=jnp.float32)
    widened = fine_vec.astype(jnp.float32)
    kinds_row = jnp.arange(KINDS, dtype=jnp.int32)
    for level_num in range(LEVELS):
        coarse_num = max(all_blocks // 4 ** (level_num + 1), 1)
        span_blocks = all_blocks // coarse_num
        run_len = min(span_blocks, BLK_DEV)
        run_num = all_blocks // run_len
        selector = pattern[level_num][:, None] == kinds_row[None, :]
        onehot = selector.astype(jnp.float32).reshape(run_num, run_len, KINDS)
        tiles = restrict[level_num].astype(jnp.float32)
        grouped = jnp.einsum("nsc,nsk->nkc", widened.reshape(run_num, run_len, width), onehot, precision=EXACT)
        grouped = grouped.astype(jnp.bfloat16).astype(jnp.float32)
        per_run = jnp.einsum("nkc,kcd->nd", grouped, tiles, precision=EXACT)
        coarse = jnp.sum(per_run.reshape(coarse_num, span_blocks // run_len, width), axis=1) * (span_blocks ** -0.5)
        rounded = coarse.astype(jnp.bfloat16)
        solved = jnp.dot(rounded, coarse_inv[level_num], preferred_element_type=jnp.float32).astype(jnp.bfloat16)
        lifted = jnp.einsum("jd,kcd->jkc", solved.astype(jnp.float32), tiles, precision=EXACT)
        kind_map = pattern[level_num].reshape(coarse_num, span_blocks)
        for kind_num in range(KINDS):
            chosen = (kind_map == kind_num)[:, :, None]
            part_add = jnp.where(chosen, lifted[:, kind_num][:, None, :], jnp.float32(0.0))
            result = result + part_add.reshape(all_blocks, width)
    return result


def reference(fine, pattern, stencil, restrict, coarse_inv):
    return lax.map(lambda fine_vec: one_vector(fine_vec, pattern, stencil, restrict, coarse_inv), fine)
```

```python
import functools

import jax
import jax.numpy as jnp
from jax import lax
from jax.experimental import pallas as pl
from jax.experimental.pallas import tpu as pltpu
from jax.sharding import PartitionSpec as P

BF = jnp.bfloat16
F32 = jnp.float32
MIB = 1 << 20


def dot(a, b):
    return jnp.dot(a, b, preferred_element_type=F32)


def vmem_spec():
    return pl.BlockSpec(memory_space=pltpu.VMEM)


def any_spec():
    return pl.BlockSpec(memory_space=pltpu.HBM)


class Plan:
    def __init__(self, devices, fine, pattern, restrict):
        self.devices = devices
        self.nv, self.blocks, self.width = fine.shape
        self.levels, self.kinds = restrict.shape[:2]
        total = self.blocks * devices
        self.spans = []
        for level in range(self.levels):
            self.spans.append(total // max(total // 4 ** (level + 1), 1))
        self.runs = [self.blocks // min(s, self.blocks) for s in self.spans]
        local = [l for l in range(self.levels) if self.spans[l] <= self.blocks]
        self.top = [l for l in range(self.levels) if self.spans[l] > self.blocks]
        self.wide = [l for l in local if self.runs[l] * self.kinds == self.blocks]
        self.mid = [l for l in local if l not in self.wide and self.runs[l] % 16 == 0]
        self.thin = [l for l in local if l not in self.wide and l not in self.mid]
        self.row = {}
        at = 0
        for l in self.mid:
            self.row[l] = at
            at += self.kinds * self.runs[l]
        self.mid_rows = at
        at = 0
        for l in self.thin + self.top:
            self.row[l] = at
            at += self.kinds * self.runs[l]
        self.first_row = at
        self.last_row = at + 1
        self.thin_rows = -(-(at + 2) // 8) * 8
        self.a_rows = -(-(self.mid_rows + self.thin_rows) // 16) * 16
        self.col = {}
        at = 0
        for l in self.mid + self.thin:
            self.col[l] = at
            at += self.kinds * self.runs[l]
        self.cols = -(-at // 128) * 128
        self.used_cols = at
        self.top_cols = self.kinds * len(self.top)

    def target(self, pat, l, base):
        index = lax.broadcasted_iota(jnp.int32, (1, self.blocks), 1)
        run = index // min(self.spans[l], self.blocks)
        return base + pat[l : l + 1, :] * self.runs[l] + run


def kernel_a(plan, fine, pattern, restrict_hbm, fine_v, g_mid, g_thin, tops, msg, hb, m1, mt1, mt2, mtop, pat_s, r_s, m_s, sems, psem, rsem):
    nv, blocks, width = plan.nv, plan.blocks, plan.width
    kinds = plan.kinds
    chunks = sems.shape[0]
    per = nv // chunks
    ntop = len(plan.top)
    pcopy = pltpu.make_async_copy(pattern, pat_s, psem)
    pcopy.start()
    copies = [
        pltpu.make_async_copy(fine.at[pl.ds(n * per, per)], fine_v.at[pl.ds(n * per, per)], sems.at[n])
        for n in range(chunks)
    ]
    for c in copies:
        c.start()
    rcopy = pltpu.make_async_copy(restrict_hbm.at[pl.ds(plan.top[0], ntop)], r_s, rsem)
    rcopy.start()
    pcopy.wait()
    pat = pat_s[...]
    rows = lax.broadcasted_iota(jnp.int32, (plan.a_rows, blocks), 0)
    hit = jnp.zeros((plan.a_rows, blocks), jnp.bool_)
    for l in plan.mid:
        hit = hit | (rows == plan.target(pat, l, plan.row[l]))
    for l in plan.thin + plan.top:
        hit = hit | (rows == plan.target(pat, l, plan.row[l] + plan.mid_rows))
    cols = lax.broadcasted_iota(jnp.int32, (plan.a_rows, blocks), 1)
    hit = hit | ((rows == plan.first_row + plan.mid_rows) & (cols == 0))
    hit = hit | ((rows == plan.last_row + plan.mid_rows) & (cols == blocks - 1))
    m_s[...] = jnp.where(hit, 1.0, 0.0).astype(BF)
    wide = plan.wide[0]
    t_wide = plan.target(pat, wide, 0)
    wrows = lax.broadcasted_iota(jnp.int32, (blocks, blocks), 0)
    m1[...] = jnp.where(wrows == t_wide, 1.0, 0.0).astype(BF)

    def column(row_vec, lanes):
        return jnp.broadcast_to(row_vec.astype(F32), (lanes, blocks)).T

    lane = lax.broadcasted_iota(jnp.int32, (blocks, 128), 1).astype(F32)
    tw = column(t_wide, 128)
    for n in range(blocks // 128):
        mt1[:, pl.ds(n * 128, 128)] = jnp.where(tw == lane + float(n * 128), 1.0, 0.0).astype(BF)
    hit2 = jnp.zeros((blocks, 128), jnp.bool_)
    for l in plan.mid + plan.thin:
        hit2 = hit2 | (column(plan.target(pat, l, plan.col[l]), 128) == lane)
    mt2[...] = jnp.where(hit2, 1.0, 0.0).astype(BF)
    hit3 = jnp.zeros((blocks, 128), jnp.bool_)
    for n, l in enumerate(plan.top):
        hit3 = hit3 | (column(pat[l : l + 1, :] + n * kinds, 128) == lane)
    mtop[...] = jnp.where(hit3, 1.0, 0.0).astype(BF)

    m = m_s[...]
    for n in range(chunks):
        copies[n].wait()
        for p in range(per // 2):
            v = n * per + 2 * p
            pair = jnp.concatenate([fine_v[v], fine_v[v + 1]], axis=1)
            g = dot(m, pair)
            for h in range(2):
                half = g[:, h * width : (h + 1) * width]
                for l in plan.mid:
                    runs = plan.runs[l]
                    for k in range(kinds):
                        r = plan.row[l] + k * runs
                        o = plan.row[l] * nv + k * runs * nv
                        g_mid[pl.ds(o + (v + h) * runs, runs), :] = half[r : r + runs].astype(BF)
                g_thin[pl.ds((v + h) * plan.thin_rows, plan.thin_rows), :] = half[
                    plan.mid_rows : plan.mid_rows + plan.thin_rows
                ]
    rcopy.wait()
    for n, l in enumerate(plan.top):
        parts = [
            g_thin[pl.ds(plan.row[l] + k, nv, stride=plan.thin_rows), :].astype(BF) for k in range(kinds)
        ]
        tile = jnp.concatenate([r_s[n, k] for k in range(kinds)], axis=0)
        coarse = dot(jnp.concatenate(parts, axis=1), tile)
        tops[n] = coarse
        msg[n] = coarse.astype(BF)
    first = g_thin[pl.ds(plan.first_row, nv, stride=plan.thin_rows), :].astype(BF)
    last = g_thin[pl.ds(plan.last_row, nv, stride=plan.thin_rows), :].astype(BF)
    odd = lax.axis_index("gx") % 2 == 1

    @pl.when(odd)
    def _():
        msg[ntop] = first
        hb[...] = last

    @pl.when(jnp.logical_not(odd))
    def _():
        msg[ntop] = last
        hb[...] = first


def chain(plan, l, parts, tiles, inverse, tiles_t):
    coarse = dot(jnp.concatenate(parts, axis=1), tiles) * plan.spans[l] ** (-0.5)
    solved = dot(coarse.astype(BF), inverse).astype(BF)
    return dot(solved, tiles_t)


def kernel_b1(plan, g_mid, g_thin, restrict, inverse, lsm):
    nv, kinds, width = plan.nv, plan.kinds, plan.width
    lv = plan.mid + plan.thin
    base = lv[0]
    lthin = g_thin
    for l in plan.mid:
        runs = plan.runs[l]
        o = plan.row[l] * nv
        tiles = jnp.concatenate([restrict[l, k] for k in range(kinds)], axis=0)
        tiles_t = jnp.concatenate([restrict[l, k].T for k in range(kinds)], axis=1)
        step = min(nv, 16)
        for s in range(0, nv, step):
            parts = [g_mid[pl.ds(o + (k * nv + s) * runs, step * runs), :] for k in range(kinds)]
            lifted = chain(plan, l, parts, tiles, inverse[l], tiles_t).astype(BF)
            for v in range(step):
                for k in range(kinds):
                    lsm[s + v, pl.ds(plan.col[l] + k * runs, runs), :] = lifted[
                        v * runs : (v + 1) * runs, k * width : (k + 1) * width
                    ]
    rows_at = plan.col[plan.thin[0]]
    blank = plan.cols - rows_at

    def body(scr):
        scr[...] = jnp.zeros_like(scr)
        for l in plan.thin:
            runs = plan.runs[l]
            tiles = jnp.concatenate([restrict[l, k] for k in range(kinds)], axis=0)
            tiles_t = jnp.concatenate([restrict[l, k].T for k in range(kinds)], axis=1)
            parts = []
            for k in range(kinds):
                rows = [
                    lthin[pl.ds(plan.row[l] + k * runs + j, nv, stride=plan.thin_rows), :].astype(BF)
                    for j in range(runs)
                ]
                parts.append(jnp.concatenate(rows, axis=0))
            lifted = chain(plan, l, parts, tiles, inverse[l], tiles_t)
            for j in range(runs):
                for k in range(kinds):
                    at = plan.col[l] - rows_at + k * runs + j
                    scr[pl.ds(at, nv, stride=blank), :] = lifted[
                        j * nv : (j + 1) * nv, k * width : (k + 1) * width
                    ]
        for v in range(nv):
            lsm[v, pl.ds(rows_at, blank), :] = scr[pl.ds(v * blank, blank), :].astype(BF)

    pl.run_scoped(body, pltpu.VMEM((nv * blank, width), F32))


def kernel_b(plan, start, count, fine_v, m1, mt1, mt2, lsm, stencil, restrict, inverse, out):
    kinds, width, blocks = plan.kinds, plan.width, plan.blocks
    l = plan.wide[0]
    runs = plan.runs[l]
    group = 4
    tiles = jnp.concatenate([restrict[l, k] for k in range(kinds)], axis=0)
    tiles_t = jnp.concatenate([restrict[l, k].T for k in range(kinds)], axis=1)
    zero = jnp.zeros((width, width), BF)
    sten = jnp.concatenate(
        [
            jnp.concatenate([stencil[1], stencil[0]], axis=1),
            jnp.concatenate([stencil[2], zero], axis=1),
        ],
        axis=0,
    )

    def body(scr, scr_t, scr_s):
        scr[...] = tiles
        scr_t[...] = tiles_t
        scr_s[...] = sten
        rowid = lax.broadcasted_iota(jnp.int32, (blocks, width), 0)

        def step(n, carry):
            v0 = start + n * group
            fs = [fine_v[v0 + q] for q in range(group)]
            gs = []
            for p in range(group // 2):
                pair = jnp.concatenate([fs[2 * p], fs[2 * p + 1]], axis=1)
                g = dot(m1[...], pair).astype(BF)
                gs.append(g[:, :width])
                gs.append(g[:, width:])
            parts = [
                jnp.concatenate([g[k * runs : (k + 1) * runs] for g in gs], axis=0) for k in range(kinds)
            ]
            lifted = chain(plan, l, parts, scr[...], inverse[l], scr_t[...]).astype(BF)
            for p in range(group // 2):
                halves = []
                for q in (2 * p, 2 * p + 1):
                    rows = [
                        lifted[q * runs : (q + 1) * runs, k * width : (k + 1) * width] for k in range(kinds)
                    ]
                    halves.append(jnp.concatenate(rows + [lsm[v0 + q]], axis=0))
                big = jnp.concatenate(halves, axis=1)
                e = dot(mt1[...], big[:blocks]) + dot(mt2[...], big[blocks:])
                for h in range(2):
                    q = 2 * p + h
                    f = fs[q].astype(F32)
                    nxt = jnp.where(rowid == blocks - 1, 0.0, pltpu.roll(f, blocks - 1, 0)).astype(BF)
                    y = dot(jnp.concatenate([fs[q], nxt], axis=1), scr_s[...])
                    prev = jnp.where(rowid == 0, 0.0, pltpu.roll(y[:, width:], 1, 0))
                    out[n * group + q] = e[:, h * width : (h + 1) * width] + y[:, :width] + prev
            return carry

        lax.fori_loop(0, count // group, step, 0)

    pl.run_scoped(
        body,
        pltpu.VMEM((kinds * width, width), BF),
        pltpu.VMEM((width, kinds * width), BF),
        pltpu.VMEM((2 * width, 2 * width), BF),
    )


def kernel_c(plan, counts, *refs):
    nparts = len(counts)
    res = refs[:nparts]
    sums, halo_r, halo_o, mtop, stencil, restrict, inverse, out = refs[nparts : nparts + 8]
    lt, h0, h2, ring, sems = refs[nparts + 8 :]
    nv, kinds, width, blocks = plan.nv, plan.kinds, plan.width, plan.blocks
    tcols = plan.top_cols
    for n, l in enumerate(plan.top):
        coarse = (sums[n] * plan.spans[l] ** (-0.5)).astype(BF)
        solved = dot(coarse, inverse[l]).astype(BF)
        tiles_t = jnp.concatenate([restrict[l, k].T for k in range(kinds)], axis=1)
        lifted = dot(solved, tiles_t)
        for k in range(kinds):
            lt[pl.ds(n * kinds + k, nv, stride=tcols), :] = lifted[:, k * width : (k + 1) * width]
    odd = lax.axis_index("gx") % 2 == 1
    hr = halo_r[...]
    ho = halo_o[...]
    h0[...] = dot(jnp.where(odd, hr, ho), stencil[0])
    h2[...] = dot(jnp.where(odd, ho, hr), stencil[2])
    slots, per = ring.shape[:2]
    mt = mtop[...][:, :tcols]

    total = 0
    for part in range(nparts):
        for n in range(counts[part] // per):
            slot = total % slots
            if total >= slots:
                pltpu.make_async_copy(ring.at[slot], out.at[pl.ds((total - slots) * per, per)], sems.at[slot]).wait()
            for p in range(per // 2):
                v = total * per + 2 * p
                pair = jnp.concatenate(
                    [lt[pl.ds(v * tcols, tcols), :], lt[pl.ds((v + 1) * tcols, tcols), :]], axis=1
                ).astype(BF)
                e = dot(mt, pair)
                for h in range(2):
                    ring[slot, 2 * p + h] = res[part][n * per + 2 * p + h] + e[:, h * width : (h + 1) * width]
                    ring[slot, 2 * p + h, pl.ds(0, 1), :] += h0[pl.ds(v + h, 1), :]
                    ring[slot, 2 * p + h, pl.ds(blocks - 1, 1), :] += h2[pl.ds(v + h, 1), :]
            pltpu.make_async_copy(ring.at[slot], out.at[pl.ds(total * per, per)], sems.at[slot]).start()
            total += 1
    for n in range(max(total - slots, 0), total):
        slot = n % slots
        pltpu.make_async_copy(ring.at[slot], out.at[pl.ds(n * per, per)], sems.at[slot]).wait()


def params(mib):
    return pltpu.CompilerParams(vmem_limit_bytes=mib * MIB)


def shards(fine, pattern, stencil, restrict, coarse_inv):
    devices = lax.axis_size("gx")
    plan = Plan(devices, fine, pattern, restrict)
    nv, blocks, width = fine.shape
    ntop = len(plan.top)
    chunks = 8
    vm = pltpu.VMEM
    a_out = (
        vm(fine.shape, BF),
        vm((plan.mid_rows * nv, width), BF),
        vm((plan.thin_rows * nv, width), F32),
        vm((ntop, nv, width), F32),
        vm((ntop + 1, nv, width), BF),
        vm((nv, width), BF),
        vm((blocks, blocks), BF),
        vm((blocks, blocks), BF),
        vm((blocks, 128), BF),
        vm((blocks, 128), BF),
    )
    fine_v, g_mid, g_thin, tops, msg, hb, m1, mt1, mt2, mtop = pl.pallas_call(
        functools.partial(kernel_a, plan),
        out_shape=a_out,
        in_specs=[any_spec(), any_spec(), any_spec()],
        out_specs=tuple(vmem_spec() for _ in a_out),
        scratch_shapes=[
            pltpu.VMEM(pattern.shape, jnp.int32),
            pltpu.VMEM((ntop,) + restrict.shape[1:], BF),
            pltpu.VMEM((plan.a_rows, blocks), BF),
            pltpu.SemaphoreType.DMA((chunks,)),
            pltpu.SemaphoreType.DMA,
            pltpu.SemaphoreType.DMA,
        ],
        compiler_params=params(12),
        name="gather_sums",
    )(fine, pattern, restrict)

    def permute(x, to):
        return lax.ppermute(x, "gx", [(i, to(i) % devices) for i in range(devices)])

    rounds = devices.bit_length() - 1
    halo_o = permute(hb, lambda i: i + 1 if i % 2 else i - 1)

    lsm = pl.pallas_call(
        functools.partial(kernel_b1, plan),
        out_shape=vm((nv, plan.cols, width), BF),
        in_specs=[vmem_spec()] * 4,
        out_specs=vmem_spec(),
        compiler_params=params(16),
        name="local_levels",
    )(g_mid, g_thin, restrict, coarse_inv)

    nparts = 4
    counts = [nv // nparts] * nparts
    parts = []
    for n in range(nparts):
        parts.append(
            pl.pallas_call(
                functools.partial(kernel_b, plan, sum(counts[:n]), counts[n]),
                out_shape=vm((counts[n], blocks, width), F32),
                in_specs=[vmem_spec()] * 8,
                out_specs=vmem_spec(),
                compiler_params=params(16),
                name="local_part",
            )(fine_v, m1, mt1, mt2, lsm, stencil, restrict, coarse_inv)
        )

    done = [None] * ntop
    live = tops
    alive = list(range(ntop))
    message = msg
    halo_r = None
    for b in range(rounds):
        flip = (1 << b) | 1
        got = permute(message, lambda i: i ^ flip)
        if b == 0:
            halo_r = got[ntop]
            got = got[:ntop]
        live = live + got.astype(F32)
        keep = [p for p in range(len(alive)) if plan.spans[plan.top[alive[p]]] // blocks > 2 << b]
        for p in range(len(alive)):
            if p not in keep:
                done[alive[p]] = live[p]
        if keep and len(keep) < len(alive):
            live = live[keep[0] :]
        alive = [alive[p] for p in keep]
        message = live.astype(BF)
    sums = jnp.stack(done)

    per = 4
    slots = 4
    return pl.pallas_call(
        functools.partial(kernel_c, plan, counts),
        out_shape=jax.ShapeDtypeStruct(fine.shape, F32),
        in_specs=[vmem_spec()] * (nparts + 7),
        out_specs=any_spec(),
        scratch_shapes=[
            pltpu.VMEM((plan.top_cols * nv, width), F32),
            pltpu.VMEM((nv, width), F32),
            pltpu.VMEM((nv, width), F32),
            pltpu.VMEM((slots, per, blocks, width), F32),
            pltpu.SemaphoreType.DMA((slots,)),
        ],
        compiler_params=params(16),
        name="finish",
    )(*parts, sums, halo_r, halo_o, mtop, stencil, restrict, coarse_inv)


def solution(mesh):
    in_specs = (P(None, "gx", None), P(None, "gx"), P(), P(), P())
    out_specs = P(None, "gx", None)
    return jax.shard_map(shards, mesh=mesh, in_specs=in_specs, out_specs=out_specs, check_vma=False)
```

```python
import functools

import jax
import jax.numpy as jnp
from jax import lax
from jax.experimental import pallas as pl
from jax.experimental.pallas import tpu as pltpu
from jax.sharding import PartitionSpec as P


BF = jnp.bfloat16
F32 = jnp.float32
MIB = 1 << 20


def dot(a, b):
    return jnp.dot(a, b, preferred_element_type=F32)


def vmem_spec():
    return pl.BlockSpec(memory_space=pltpu.VMEM)


def any_spec():
    return pl.BlockSpec(memory_space=pltpu.HBM)


class Plan:
    def __init__(self, devices, fine, restrict):
        self.nv, self.blocks, self.width = fine.shape
        self.levels, self.kinds = restrict.shape[:2]
        total = self.blocks * devices
        self.spans = []
        for level in range(self.levels):
            self.spans.append(total // max(total // 4 ** (level + 1), 1))
        self.runs = [self.blocks // min(s, self.blocks) for s in self.spans]
        local = [l for l in range(self.levels) if self.spans[l] <= self.blocks]
        self.top = [l for l in range(self.levels) if self.spans[l] > self.blocks]
        self.wide = [l for l in local if self.runs[l] * self.kinds == self.blocks]
        self.mid = [l for l in local if l not in self.wide and self.runs[l] % 16 == 0]
        self.thin = [l for l in local if l not in self.wide and l not in self.mid]
        self.row = {}
        at = 0
        for l in self.mid:
            self.row[l] = at
            at += self.kinds * self.runs[l]
        self.mid_rows = at
        at = 0
        for l in self.thin + self.top:
            self.row[l] = at
            at += self.kinds * self.runs[l]
        self.first_row = at
        self.last_row = at + 1
        self.thin_rows = -(-(at + 2) // 8) * 8
        self.a_rows = -(-(self.mid_rows + self.thin_rows) // 16) * 16
        self.col = {}
        at = 0
        for l in self.mid + self.thin:
            self.col[l] = at
            at += self.kinds * self.runs[l]
        self.cols = -(-at // 128) * 128
        self.top_cols = self.kinds * len(self.top)

    def target(self, pat, l, base):
        index = lax.broadcasted_iota(jnp.int32, (1, self.blocks), 1)
        run = index // min(self.spans[l], self.blocks)
        return base + pat[l : l + 1, :] * self.runs[l] + run


def kernel_a(plan, fine, pattern, restrict_hbm, fine_v, g_mid, g_thin, tops, msg, hb, m1, mt1, mt2, mtop, pat_s, r_s, m_s, sems, psem, rsem):
    nv, blocks, width = plan.nv, plan.blocks, plan.width
    kinds = plan.kinds
    chunks = sems.shape[0]
    per = nv // chunks
    ntop = len(plan.top)
    pcopy = pltpu.make_async_copy(pattern, pat_s, psem)
    pcopy.start()
    copies = [
        pltpu.make_async_copy(fine.at[pl.ds(n * per, per)], fine_v.at[pl.ds(n * per, per)], sems.at[n])
        for n in range(chunks)
    ]
    for c in copies:
        c.start()
    rcopy = pltpu.make_async_copy(restrict_hbm.at[pl.ds(plan.top[0], ntop)], r_s, rsem)
    rcopy.start()
    pcopy.wait()
    pat = pat_s[...]
    rows = lax.broadcasted_iota(jnp.int32, (plan.a_rows, blocks), 0)
    hit = jnp.zeros((plan.a_rows, blocks), jnp.bool_)
    for l in plan.mid:
        hit = hit | (rows == plan.target(pat, l, plan.row[l]))
    for l in plan.thin + plan.top:
        hit = hit | (rows == plan.target(pat, l, plan.row[l] + plan.mid_rows))
    cols = lax.broadcasted_iota(jnp.int32, (plan.a_rows, blocks), 1)
    hit = hit | ((rows == plan.first_row + plan.mid_rows) & (cols == 0))
    hit = hit | ((rows == plan.last_row + plan.mid_rows) & (cols == blocks - 1))
    m_s[...] = jnp.where(hit, 1.0, 0.0).astype(BF)
    wide = plan.wide[0]
    t_wide = plan.target(pat, wide, 0)
    wrows = lax.broadcasted_iota(jnp.int32, (blocks, blocks), 0)
    m1[...] = jnp.where(wrows == t_wide, 1.0, 0.0).astype(BF)

    def column(row_vec, lanes):
        return jnp.broadcast_to(row_vec.astype(F32), (lanes, blocks)).T

    lane = lax.broadcasted_iota(jnp.int32, (blocks, 128), 1).astype(F32)
    tw = column(t_wide, 128)
    for n in range(blocks // 128):
        mt1[:, pl.ds(n * 128, 128)] = jnp.where(tw == lane + float(n * 128), 1.0, 0.0).astype(BF)
    hit2 = jnp.zeros((blocks, 128), jnp.bool_)
    for l in plan.mid + plan.thin:
        hit2 = hit2 | (column(plan.target(pat, l, plan.col[l]), 128) == lane)
    mt2[...] = jnp.where(hit2, 1.0, 0.0).astype(BF)
    hit3 = jnp.zeros((blocks, 128), jnp.bool_)
    for n, l in enumerate(plan.top):
        hit3 = hit3 | (column(pat[l : l + 1, :] + n * kinds, 128) == lane)
    mtop[...] = jnp.where(hit3, 1.0, 0.0).astype(BF)

    m = m_s[...]
    for n in range(chunks):
        copies[n].wait()
        for p in range(per // 2):
            v = n * per + 2 * p
            pair = jnp.concatenate([fine_v[v], fine_v[v + 1]], axis=1)
            g = dot(m, pair)
            for h in range(2):
                half = g[:, h * width : (h + 1) * width]
                for l in plan.mid:
                    runs = plan.runs[l]
                    for k in range(kinds):
                        r = plan.row[l] + k * runs
                        o = plan.row[l] * nv + k * runs * nv
                        g_mid[pl.ds(o + (v + h) * runs, runs), :] = half[r : r + runs].astype(BF)
                g_thin[pl.ds((v + h) * plan.thin_rows, plan.thin_rows), :] = half[
                    plan.mid_rows : plan.mid_rows + plan.thin_rows
                ]
    rcopy.wait()
    for n, l in enumerate(plan.top):
        parts = [
            g_thin[pl.ds(plan.row[l] + k, nv, stride=plan.thin_rows), :].astype(BF) for k in range(kinds)
        ]
        tile = jnp.concatenate([r_s[n, k] for k in range(kinds)], axis=0)
        coarse = dot(jnp.concatenate(parts, axis=1), tile)
        tops[n] = coarse
        msg[n] = coarse.astype(BF)
    first = g_thin[pl.ds(plan.first_row, nv, stride=plan.thin_rows), :].astype(BF)
    last = g_thin[pl.ds(plan.last_row, nv, stride=plan.thin_rows), :].astype(BF)
    odd = lax.axis_index("gx") % 2 == 1

    @pl.when(odd)
    def _():
        msg[ntop] = first
        hb[...] = last

    @pl.when(jnp.logical_not(odd))
    def _():
        msg[ntop] = last
        hb[...] = first


def chain(plan, l, parts, tiles, inverse, tiles_t):
    coarse = dot(jnp.concatenate(parts, axis=1), tiles) * plan.spans[l] ** (-0.5)
    solved = dot(coarse.astype(BF), inverse).astype(BF)
    return dot(solved, tiles_t)


def kernel_b1(plan, g_mid, g_thin, restrict, inverse, lsm):
    nv, kinds, width = plan.nv, plan.kinds, plan.width
    lthin = g_thin
    for l in plan.mid:
        runs = plan.runs[l]
        o = plan.row[l] * nv
        tiles = jnp.concatenate([restrict[l, k] for k in range(kinds)], axis=0)
        tiles_t = jnp.concatenate([restrict[l, k].T for k in range(kinds)], axis=1)
        step = min(nv, 16)
        for s in range(0, nv, step):
            parts = [g_mid[pl.ds(o + (k * nv + s) * runs, step * runs), :] for k in range(kinds)]
            lifted = chain(plan, l, parts, tiles, inverse[l], tiles_t).astype(BF)
            for v in range(step):
                for k in range(kinds):
                    lsm[s + v, pl.ds(plan.col[l] + k * runs, runs), :] = lifted[
                        v * runs : (v + 1) * runs, k * width : (k + 1) * width
                    ]
    rows_at = plan.col[plan.thin[0]]
    blank = plan.cols - rows_at

    def body(scr):
        scr[...] = jnp.zeros_like(scr)
        for l in plan.thin:
            runs = plan.runs[l]
            tiles = jnp.concatenate([restrict[l, k] for k in range(kinds)], axis=0)
            tiles_t = jnp.concatenate([restrict[l, k].T for k in range(kinds)], axis=1)
            parts = []
            for k in range(kinds):
                rows = [
                    lthin[pl.ds(plan.row[l] + k * runs + j, nv, stride=plan.thin_rows), :].astype(BF)
                    for j in range(runs)
                ]
                parts.append(jnp.concatenate(rows, axis=0))
            lifted = chain(plan, l, parts, tiles, inverse[l], tiles_t)
            for j in range(runs):
                for k in range(kinds):
                    at = plan.col[l] - rows_at + k * runs + j
                    scr[pl.ds(at, nv, stride=blank), :] = lifted[
                        j * nv : (j + 1) * nv, k * width : (k + 1) * width
                    ]
        for v in range(nv):
            lsm[v, pl.ds(rows_at, blank), :] = scr[pl.ds(v * blank, blank), :].astype(BF)

    pl.run_scoped(body, pltpu.VMEM((nv * blank, width), F32))


def kernel_b(plan, start, count, fine_v, m1, mt1, mt2, lsm, stencil, restrict, inverse, out):
    kinds, width, blocks = plan.kinds, plan.width, plan.blocks
    l = plan.wide[0]
    runs = plan.runs[l]
    group = 4
    tiles = jnp.concatenate([restrict[l, k] for k in range(kinds)], axis=0)
    tiles_t = jnp.concatenate([restrict[l, k].T for k in range(kinds)], axis=1)
    zero = jnp.zeros((width, width), BF)
    sten = jnp.concatenate(
        [
            jnp.concatenate([stencil[1], stencil[0]], axis=1),
            jnp.concatenate([stencil[2], zero], axis=1),
        ],
        axis=0,
    )

    def body(scr, scr_t, scr_s):
        scr[...] = tiles
        scr_t[...] = tiles_t
        scr_s[...] = sten
        rowid = lax.broadcasted_iota(jnp.int32, (blocks, width), 0)

        def step(n, carry):
            v0 = start + n * group
            fs = [fine_v[v0 + q] for q in range(group)]
            gs = []
            for p in range(group // 2):
                pair = jnp.concatenate([fs[2 * p], fs[2 * p + 1]], axis=1)
                g = dot(m1[...], pair).astype(BF)
                gs.append(g[:, :width])
                gs.append(g[:, width:])
            parts = [
                jnp.concatenate([g[k * runs : (k + 1) * runs] for g in gs], axis=0) for k in range(kinds)
            ]
            lifted = chain(plan, l, parts, scr[...], inverse[l], scr_t[...]).astype(BF)
            for p in range(group // 2):
                halves = []
                for q in (2 * p, 2 * p + 1):
                    rows = [
                        lifted[q * runs : (q + 1) * runs, k * width : (k + 1) * width] for k in range(kinds)
                    ]
                    halves.append(jnp.concatenate(rows + [lsm[v0 + q]], axis=0))
                big = jnp.concatenate(halves, axis=1)
                e = dot(mt1[...], big[:blocks]) + dot(mt2[...], big[blocks:])
                for h in range(2):
                    q = 2 * p + h
                    f = fs[q].astype(F32)
                    nxt = jnp.where(rowid == blocks - 1, 0.0, pltpu.roll(f, blocks - 1, 0)).astype(BF)
                    y = dot(jnp.concatenate([fs[q], nxt], axis=1), scr_s[...])
                    prev = jnp.where(rowid == 0, 0.0, pltpu.roll(y[:, width:], 1, 0))
                    out[n * group + q] = e[:, h * width : (h + 1) * width] + y[:, :width] + prev
            return carry

        lax.fori_loop(0, count // group, step, 0)

    pl.run_scoped(
        body,
        pltpu.VMEM((kinds * width, width), BF),
        pltpu.VMEM((width, kinds * width), BF),
        pltpu.VMEM((2 * width, 2 * width), BF),
    )


def kernel_c(plan, counts, *refs):
    nparts = len(counts)
    res = refs[:nparts]
    sums, halo_r, halo_o, mtop, stencil, restrict, inverse, out = refs[nparts : nparts + 8]
    lt, h0, h2, ring, sems = refs[nparts + 8 :]
    nv, kinds, width, blocks = plan.nv, plan.kinds, plan.width, plan.blocks
    tcols = plan.top_cols
    for n, l in enumerate(plan.top):
        coarse = (sums[n] * plan.spans[l] ** (-0.5)).astype(BF)
        solved = dot(coarse, inverse[l]).astype(BF)
        tiles_t = jnp.concatenate([restrict[l, k].T for k in range(kinds)], axis=1)
        lifted = dot(solved, tiles_t)
        for k in range(kinds):
            lt[pl.ds(n * kinds + k, nv, stride=tcols), :] = lifted[:, k * width : (k + 1) * width]
    odd = lax.axis_index("gx") % 2 == 1
    hr = halo_r[...]
    ho = halo_o[...]
    h0[...] = dot(jnp.where(odd, hr, ho), stencil[0])
    h2[...] = dot(jnp.where(odd, ho, hr), stencil[2])
    slots, per = ring.shape[:2]
    mt = mtop[...][:, :tcols]

    total = 0
    for part in range(nparts):
        for n in range(counts[part] // per):
            slot = total % slots
            if total >= slots:
                pltpu.make_async_copy(ring.at[slot], out.at[pl.ds((total - slots) * per, per)], sems.at[slot]).wait()
            for p in range(per // 2):
                v = total * per + 2 * p
                pair = jnp.concatenate(
                    [lt[pl.ds(v * tcols, tcols), :], lt[pl.ds((v + 1) * tcols, tcols), :]], axis=1
                ).astype(BF)
                e = dot(mt, pair)
                for h in range(2):
                    ring[slot, 2 * p + h] = res[part][n * per + 2 * p + h] + e[:, h * width : (h + 1) * width]
                    ring[slot, 2 * p + h, pl.ds(0, 1), :] += h0[pl.ds(v + h, 1), :]
                    ring[slot, 2 * p + h, pl.ds(blocks - 1, 1), :] += h2[pl.ds(v + h, 1), :]
            pltpu.make_async_copy(ring.at[slot], out.at[pl.ds(total * per, per)], sems.at[slot]).start()
            total += 1
    for n in range(max(total - slots, 0), total):
        slot = n % slots
        pltpu.make_async_copy(ring.at[slot], out.at[pl.ds(n * per, per)], sems.at[slot]).wait()


def params(mib):
    return pltpu.CompilerParams(vmem_limit_bytes=mib * MIB)


def shards(fine, pattern, stencil, restrict, coarse_inv):
    devices = lax.axis_size("gx")
    plan = Plan(devices, fine, restrict)
    nv, blocks, width = fine.shape
    ntop = len(plan.top)
    chunks = 8
    vm = pltpu.VMEM
    a_out = (
        vm(fine.shape, BF),
        vm((plan.mid_rows * nv, width), BF),
        vm((plan.thin_rows * nv, width), F32),
        vm((ntop, nv, width), F32),
        vm((ntop + 1, nv, width), BF),
        vm((nv, width), BF),
        vm((blocks, blocks), BF),
        vm((blocks, blocks), BF),
        vm((blocks, 128), BF),
        vm((blocks, 128), BF),
    )
    fine_v, g_mid, g_thin, tops, msg, hb, m1, mt1, mt2, mtop = pl.pallas_call(
        functools.partial(kernel_a, plan),
        out_shape=a_out,
        in_specs=[any_spec(), any_spec(), any_spec()],
        out_specs=tuple(vmem_spec() for _ in a_out),
        scratch_shapes=[
            pltpu.VMEM(pattern.shape, jnp.int32),
            pltpu.VMEM((ntop,) + restrict.shape[1:], BF),
            pltpu.VMEM((plan.a_rows, blocks), BF),
            pltpu.SemaphoreType.DMA((chunks,)),
            pltpu.SemaphoreType.DMA,
            pltpu.SemaphoreType.DMA,
        ],
        compiler_params=params(12),
        name="gather_sums",
    )(
        pltpu.with_memory_space_constraint(fine, pltpu.HBM),
        pltpu.with_memory_space_constraint(pattern, pltpu.HBM),
        pltpu.with_memory_space_constraint(restrict, pltpu.HBM),
    )

    def permute(x, to):
        return lax.ppermute(x, "gx", [(i, to(i) % devices) for i in range(devices)])

    rounds = devices.bit_length() - 1
    halo_o = permute(hb, lambda i: i + 1 if i % 2 else i - 1)

    lsm = pl.pallas_call(
        functools.partial(kernel_b1, plan),
        out_shape=vm((nv, plan.cols, width), BF),
        in_specs=[vmem_spec()] * 4,
        out_specs=vmem_spec(),
        compiler_params=params(16),
        name="local_levels",
    )(g_mid, g_thin, restrict, coarse_inv)

    nparts = 4
    counts = [nv // nparts] * nparts
    parts = []
    for n in range(nparts):
      parts.append(
          pl.pallas_call(
              functools.partial(kernel_b, plan, sum(counts[:n]), counts[n]),
              out_shape=vm((counts[n], blocks, width), F32),
              in_specs=[vmem_spec()] * 8,
              out_specs=vmem_spec(),
              compiler_params=params(16),
              name="local_part",
          )(fine_v, m1, mt1, mt2, lsm, stencil, restrict, coarse_inv)
      )

    done = [None] * ntop
    live = tops
    alive = list(range(ntop))
    message = msg
    halo_r = None
    for b in range(rounds):
        flip = (1 << b) | 1
        got = permute(message, lambda i: i ^ flip)
        if b == 0:
            halo_r = got[ntop]
            got = got[:ntop]
        live = live + got.astype(F32)
        keep = [p for p in range(len(alive)) if plan.spans[plan.top[alive[p]]] // blocks > 2 << b]
        for p in range(len(alive)):
            if p not in keep:
                done[alive[p]] = live[p]
        if keep and len(keep) < len(alive):
            live = live[keep[0] :]
        alive = [alive[p] for p in keep]
        message = live.astype(BF)
    sums = jnp.stack(done)

    per = 4
    slots = 4
    return pl.pallas_call(
        functools.partial(kernel_c, plan, counts),
        out_shape=jax.ShapeDtypeStruct(fine.shape, F32),
        in_specs=[vmem_spec()] * (nparts + 7),
        out_specs=any_spec(),
        scratch_shapes=[
            pltpu.VMEM((plan.top_cols * nv, width), F32),
            pltpu.VMEM((nv, width), F32),
            pltpu.VMEM((nv, width), F32),
            pltpu.VMEM((slots, per, blocks, width), F32),
            pltpu.SemaphoreType.DMA((slots,)),
        ],
        compiler_params=params(16),
        name="finish",
    )(*parts, sums, halo_r, halo_o, mtop, stencil, restrict, coarse_inv)


def solution(mesh):
    in_specs = (P(None, "gx", None), P(None, "gx"), P(), P(), P())
    out_specs = P(None, "gx", None)

    return jax.shard_map(shards, mesh=mesh, in_specs=in_specs, out_specs=out_specs, check_vma=False)
```

```python
import functools

import jax
import jax.numpy as jnp
from jax import lax
from jax.experimental import pallas as pl
from jax.experimental.pallas import tpu as pltpu
from jax.sharding import PartitionSpec as P


BF = jnp.bfloat16
F32 = jnp.float32
MIB = 1 << 20
PARTS = (4, 4, 4, 4)
CHUNKS = (6, 4, 4, 2)
GROUP = 8


def dot(a, b):
    return jnp.dot(a, b, preferred_element_type=F32)


def vmem_spec():
    return pl.BlockSpec(memory_space=pltpu.VMEM)


def any_spec():
    return pl.BlockSpec(memory_space=pltpu.HBM)


class Plan:
    def __init__(self, devices, fine, restrict):
        self.nv, self.blocks, self.width = fine.shape
        self.levels, self.kinds = restrict.shape[:2]
        total = self.blocks * devices
        self.spans = []
        for level in range(self.levels):
            self.spans.append(total // max(total // 4 ** (level + 1), 1))
        self.runs = [self.blocks // min(s, self.blocks) for s in self.spans]
        local = [l for l in range(self.levels) if self.spans[l] <= self.blocks]
        self.top = [l for l in range(self.levels) if self.spans[l] > self.blocks]
        self.wide = [l for l in local if self.runs[l] * self.kinds == self.blocks]
        self.mid = [l for l in local if l not in self.wide and self.runs[l] % 16 == 0]
        self.thin = [l for l in local if l not in self.wide and l not in self.mid]
        self.row = {}
        at = 0
        for l in self.mid:
            self.row[l] = at
            at += self.kinds * self.runs[l]
        self.mid_rows = at
        at = 0
        for l in self.thin + self.top:
            self.row[l] = at
            at += self.kinds * self.runs[l]
        self.first_row = at
        self.last_row = at + 1
        self.thin_rows = -(-(at + 2) // 8) * 8
        self.a_rows = -(-(self.mid_rows + self.thin_rows) // 16) * 16
        self.col = {}
        at = 0
        for l in self.mid + self.thin:
            self.col[l] = at
            at += self.kinds * self.runs[l]
        self.cols = -(-at // 128) * 128
        self.used_cols = at
        self.top_cols = self.kinds * len(self.top)

    def target(self, pat, l, base):
        index = lax.broadcasted_iota(jnp.int32, (1, self.blocks), 1)
        run = index // min(self.spans[l], self.blocks)
        return base + pat[l : l + 1, :] * self.runs[l] + run


def onehot(hit):
    return jnp.where(hit, 1.0, 0.0)


def kernel_a(plan, fine, pattern, restrict, inverse, stencil, fine_v, g_mid, g_thin, tops, msg, hb, m1, mt1, mt2, mtop, r_v, inv_v, sten_v, pat_s, m_s, sems, psem, wsem):
    nv, blocks, width = plan.nv, plan.blocks, plan.width
    kinds = plan.kinds
    ntop = len(plan.top)
    sizes = [nv * c // sum(CHUNKS) for c in CHUNKS]
    chunks = len(sizes)

    def chunk_copy(n):
        at = pl.ds(sum(sizes[:n]), sizes[n])
        return pltpu.make_async_copy(fine.at[at], fine_v.at[at], sems.at[n])

    pcopy = pltpu.make_async_copy(pattern, pat_s, psem)
    pcopy.start()
    for n in range(chunks):
        chunk_copy(n).start()
    at = pl.ds(plan.top[0], ntop)
    below = pl.ds(0, plan.top[0])
    weights = [
        pltpu.make_async_copy(restrict.at[at], r_v.at[at], wsem.at[0]),
        pltpu.make_async_copy(restrict.at[below], r_v.at[below], wsem.at[1]),
        pltpu.make_async_copy(inverse, inv_v, wsem.at[2]),
        pltpu.make_async_copy(stencil, sten_v, wsem.at[3]),
    ]
    for w in weights:
        w.start()
    pcopy.wait()
    pat = pat_s[...]
    rows = lax.broadcasted_iota(jnp.int32, (plan.mid_rows, blocks), 0)
    hit = rows == plan.target(pat, plan.mid[0], plan.row[plan.mid[0]])
    for l in plan.mid[1:]:
        hit = hit | (rows == plan.target(pat, l, plan.row[l]))
    m_s[pl.ds(0, plan.mid_rows), :] = onehot(hit).astype(BF)
    rest = plan.a_rows - plan.mid_rows
    rows = lax.broadcasted_iota(jnp.int32, (rest, blocks), 0)
    cols = lax.broadcasted_iota(jnp.int32, (rest, blocks), 1)
    hit = ((rows == plan.first_row) & (cols == 0)) | ((rows == plan.last_row) & (cols == blocks - 1))
    for l in plan.thin + plan.top:
        hit = hit | (rows == plan.target(pat, l, plan.row[l]))
    m_s[pl.ds(plan.mid_rows, rest), :] = onehot(hit).astype(BF)

    t_wide = plan.target(pat, plan.wide[0], 0)
    wrows = lax.broadcasted_iota(jnp.int32, (blocks, blocks), 0)
    m1[...] = onehot(wrows == t_wide).astype(BF)
    lane = lax.broadcasted_iota(jnp.int32, (blocks, 128), 1).astype(F32)
    tw = jnp.broadcast_to(t_wide.astype(F32), (128, blocks)).T
    for n in range(blocks // 128):
        mt1[:, pl.ds(n * 128, 128)] = onehot(tw == lane + float(n * 128)).astype(BF)
    rows = lax.broadcasted_iota(jnp.int32, (plan.cols, blocks), 0)
    hit = jnp.zeros(rows.shape, jnp.bool_)
    for l in plan.mid + plan.thin:
        hit = hit | (rows == plan.target(pat, l, plan.col[l]))
    mt2[...] = onehot(hit).T.astype(BF)
    rows = lax.broadcasted_iota(jnp.int32, (128, blocks), 0)
    hit = jnp.zeros(rows.shape, jnp.bool_)
    for n, l in enumerate(plan.top):
        hit = hit | (rows == pat[l : l + 1, :] + n * kinds)
    mtop[...] = onehot(hit).T.astype(BF)
    m = m_s[...]
    for n in range(chunks):
        chunk_copy(n).wait()
        for p in range(sizes[n] // 2):
            v = sum(sizes[:n]) + 2 * p
            pair = jnp.concatenate([fine_v[v], fine_v[v + 1]], axis=1)
            g = dot(m, pair)
            for h in range(2):
                half = g[:, h * width : (h + 1) * width]
                for l in plan.mid:
                    runs = plan.runs[l]
                    for k in range(kinds):
                        r = plan.row[l] + k * runs
                        o = plan.row[l] * nv + k * runs * nv
                        g_mid[pl.ds(o + (v + h) * runs, runs), :] = half[r : r + runs].astype(BF)
                g_thin[pl.ds((v + h) * plan.thin_rows, plan.thin_rows), :] = half[
                    plan.mid_rows : plan.mid_rows + plan.thin_rows
                ]
    weights[0].wait()
    for n, l in enumerate(plan.top):
        parts = [
            g_thin[pl.ds(plan.row[l] + k, nv, stride=plan.thin_rows), :].astype(BF) for k in range(kinds)
        ]
        tile = flat(r_v, l, kinds)
        coarse = dot(jnp.concatenate(parts, axis=1), tile)
        tops[n] = coarse
        msg[n] = coarse.astype(BF)
    first = g_thin[pl.ds(plan.first_row, nv, stride=plan.thin_rows), :].astype(BF)
    last = g_thin[pl.ds(plan.last_row, nv, stride=plan.thin_rows), :].astype(BF)
    odd = lax.axis_index("gx") % 2 == 1
    msg[ntop] = jnp.where(odd, first, last)
    hb[...] = jnp.where(odd, last, first)

    for w in weights[1:]:
        w.wait()


def flat(restrict, l, kinds):
    return jnp.concatenate([restrict[l, k] for k in range(kinds)], axis=0)


def flat_t(restrict, l, kinds):
    return jnp.concatenate([restrict[l, k].T for k in range(kinds)], axis=1)


def chain(plan, l, parts, tiles, inverse, tiles_t):
    coarse = dot(jnp.concatenate(parts, axis=1), tiles) * plan.spans[l] ** (-0.5)
    solved = dot(coarse.astype(BF), inverse).astype(BF)
    return dot(solved, tiles_t)


def kernel_b1(plan, g_mid, g_thin, restrict, inverse, lsm, t_wide, rt_top, scr):
    nv, kinds, width = plan.nv, plan.kinds, plan.width
    l = plan.wide[0]
    w = dot(flat(restrict, l, kinds), inverse[l]) * plan.spans[l] ** (-0.5)
    high = w.astype(BF)
    low = (w - high.astype(F32)).astype(BF)
    tiles_t = flat_t(restrict, l, kinds)
    t_wide[...] = (dot(high, tiles_t) + dot(low, tiles_t)).astype(BF)
    for n, l in enumerate(plan.top):
        rt_top[n] = flat_t(restrict, l, kinds)
    for l in plan.mid:
        runs = plan.runs[l]
        o = plan.row[l] * nv
        tiles = flat(restrict, l, kinds)
        tiles_t = flat_t(restrict, l, kinds)
        step = min(nv, 16)

        def mid_step(n, carry, l=l, runs=runs, o=o, tiles=tiles, tiles_t=tiles_t):
            parts = [
                g_mid[pl.ds(o + k * nv * runs + n * (step * runs), step * runs), :]
                for k in range(kinds)
            ]
            lifted = chain(plan, l, parts, tiles, inverse[l], tiles_t).astype(BF)
            for v in range(step):
                for k in range(kinds):
                    lsm[n * step + v, pl.ds(plan.col[l] + k * runs, runs), :] = lifted[
                        v * runs : (v + 1) * runs, k * width : (k + 1) * width
                    ]
            return carry

        for n in range(nv // step):
            mid_step(n, 0)
    rows_at = plan.col[plan.thin[0]]
    thin_cols = plan.used_cols - rows_at
    padded = -(-thin_cols // 8) * 8
    for l in plan.thin:
        runs = plan.runs[l]
        parts = []
        for k in range(kinds):
            rows = [
                g_thin[pl.ds(plan.row[l] + k * runs + j, nv, stride=plan.thin_rows), :].astype(BF)
                for j in range(runs)
            ]
            parts.append(jnp.concatenate(rows, axis=0))
        lifted = chain(plan, l, parts, flat(restrict, l, kinds), inverse[l], flat_t(restrict, l, kinds))
        for j in range(runs):
            for k in range(kinds):
                at = plan.col[l] - rows_at + k * runs + j
                scr[pl.ds(at * nv, nv), :] = lifted[j * nv : (j + 1) * nv, k * width : (k + 1) * width]
    for at in range(thin_cols, padded):
        scr[pl.ds(at * nv, nv), :] = jnp.zeros((nv, width), F32)
    pad = jnp.zeros((plan.cols - rows_at - padded, width), F32)

    def spread(n, carry):
        for q in range(8):
            v = n * 8 + q
            rows = scr[pl.ds(v, padded, stride=nv), :]
            lsm[v, pl.ds(rows_at, plan.cols - rows_at), :] = jnp.concatenate([rows, pad], axis=0).astype(BF)
        return carry

    for n in range(nv // 8):
        spread(n, 0)


def kernel_b(plan, start, count, fine_v, m1, mt1, mt2, lsm, stencil, t_wide, *refs):
    out, scr_s = refs[-2:]
    kinds, width, blocks = plan.kinds, plan.width, plan.blocks
    l = plan.wide[0]
    runs = plan.runs[l]
    group = GROUP
    scr_s[:width, :width] = stencil[1]
    scr_s[:width, width:] = stencil[0]
    scr_s[width:, :width] = stencil[2]
    scr_s[width:, width:] = jnp.zeros((width, width), BF)
    rowid = lax.broadcasted_iota(jnp.int32, (blocks, width), 0)

    def step(n, carry):
        v0 = start + n * group
        fs = [fine_v[v0 + q] for q in range(group)]
        gs = []
        for p in range(group // 2):
            pair = jnp.concatenate([fs[2 * p], fs[2 * p + 1]], axis=1)
            g = dot(m1[...], pair).astype(BF)
            gs.append(g[:, :width])
            gs.append(g[:, width:])
        parts = [
            jnp.concatenate([g[k * runs : (k + 1) * runs] for g in gs], axis=0) for k in range(kinds)
        ]
        lifted = dot(jnp.concatenate(parts, axis=1), t_wide[...]).astype(BF)
        for p in range(group // 2):
            halves = []
            for q in (2 * p, 2 * p + 1):
                rows = [
                    lifted[q * runs : (q + 1) * runs, k * width : (k + 1) * width] for k in range(kinds)
                ]
                halves.append(jnp.concatenate(rows + [lsm[v0 + q]], axis=0))
            big = jnp.concatenate(halves, axis=1)
            e = dot(mt1[...], big[:blocks]) + dot(mt2[...], big[blocks:])
            for h in range(2):
                q = 2 * p + h
                f = fs[q].astype(F32)
                nxt = jnp.where(rowid == blocks - 1, 0.0, pltpu.roll(f, blocks - 1, 0)).astype(BF)
                y = dot(jnp.concatenate([fs[q], nxt], axis=1), scr_s[...])
                prev = jnp.where(rowid == 0, 0.0, pltpu.roll(y[:, width:], 1, 0))
                out[v0 + q] = e[:, h * width : (h + 1) * width] + y[:, :width] + prev
        return carry

    lax.fori_loop(0, count // group, step, 0)


def kernel_c(plan, res, sums, halo_r, halo_o, mtop, stencil, rt_top, inverse, out, lt, h0, h2, ring, sems):
    nv, kinds, width, blocks = plan.nv, plan.kinds, plan.width, plan.blocks
    tcols = plan.top_cols
    for n, l in enumerate(plan.top):
        coarse = (sums[n] * plan.spans[l] ** (-0.5)).astype(BF)
        solved = dot(coarse, inverse[l]).astype(BF)
        lifted = dot(solved, rt_top[n])
        for k in range(kinds):
            lt[pl.ds((n * kinds + k) * nv, nv), :] = lifted[:, k * width : (k + 1) * width]
    odd = lax.axis_index("gx") % 2 == 1
    hr = halo_r[...]
    ho = halo_o[...]
    h0[...] = dot(jnp.where(odd, hr, ho), stencil[0])
    h2[...] = dot(jnp.where(odd, ho, hr), stencil[2])
    steps, per = ring.shape[:2]

    def copy(n):
        return pltpu.make_async_copy(ring.at[n], out.at[pl.ds(n * per, per)], sems.at[n])

    mt = mtop[...][:, :tcols]
    for n in range(steps):
        for p in range(per // 2):
            v = n * per + 2 * p
            pair = jnp.concatenate(
                [lt[pl.ds(v, tcols, stride=nv), :], lt[pl.ds(v + 1, tcols, stride=nv), :]], axis=1
            ).astype(BF)
            e = dot(mt, pair)
            for h in range(2):
                ring[n, 2 * p + h] = res[v + h] + e[:, h * width : (h + 1) * width]
                ring[n, 2 * p + h, pl.ds(0, 1), :] += h0[pl.ds(v + h, 1), :]
                ring[n, 2 * p + h, pl.ds(blocks - 1, 1), :] += h2[pl.ds(v + h, 1), :]
        copy(n).start()
    for n in range(steps):
        copy(n).wait()


def params(mib):
    return pltpu.CompilerParams(vmem_limit_bytes=mib * MIB)


def shards(fine, pattern, stencil, restrict, coarse_inv):
    devices = lax.axis_size("gx")
    plan = Plan(devices, fine, restrict)
    nv, blocks, width = fine.shape
    ntop = len(plan.top)
    chunks = len(CHUNKS)
    vm = pltpu.VMEM
    a_out = (
        vm(fine.shape, BF),
        vm((plan.mid_rows * nv, width), BF),
        vm((plan.thin_rows * nv, width), F32),
        vm((ntop, nv, width), F32),
        vm((ntop + 1, nv, width), BF),
        vm((nv, width), BF),
        vm((blocks, blocks), BF),
        vm((blocks, blocks), BF),
        vm((blocks, 128), BF),
        vm((blocks, 128), BF),
        vm(restrict.shape, BF),
        vm(coarse_inv.shape, BF),
        vm(stencil.shape, BF),
    )
    fine_v, g_mid, g_thin, tops, msg, hb, m1, mt1, mt2, mtop, r_v, inv_v, sten_v = pl.pallas_call(
        functools.partial(kernel_a, plan),
        out_shape=a_out,
        in_specs=[any_spec()] * 5,
        out_specs=tuple(vmem_spec() for _ in a_out),
        scratch_shapes=[
            pltpu.VMEM(pattern.shape, jnp.int32),
            pltpu.VMEM((plan.a_rows, blocks), BF),
            pltpu.SemaphoreType.DMA((chunks,)),
            pltpu.SemaphoreType.DMA,
            pltpu.SemaphoreType.DMA((4,)),
        ],
        compiler_params=params(12),
        name="gather_sums",
    )(*(pltpu.with_memory_space_constraint(x, pltpu.HBM) for x in (fine, pattern, restrict, coarse_inv, stencil)))

    def permute(x, to):
        return lax.ppermute(x, "gx", [(i, to(i) % devices) for i in range(devices)])

    rounds = devices.bit_length() - 1
    halo_o = permute(hb, lambda i: i + 1 if i % 2 else i - 1)

    lsm, t_wide, rt_top = pl.pallas_call(
        functools.partial(kernel_b1, plan),
        out_shape=(
            vm((nv, plan.cols, width), BF),
            vm((plan.kinds * width, plan.kinds * width), BF),
            vm((ntop, width, plan.kinds * width), BF),
        ),
        in_specs=[vmem_spec()] * 4,
        out_specs=(vmem_spec(),) * 3,
        scratch_shapes=[pltpu.VMEM((32 * nv, width), F32)],
        compiler_params=params(16),
        name="local_levels",
    )(g_mid, g_thin, r_v, inv_v)

    weights = PARTS
    counts = [nv * w // sum(weights) for w in weights]
    result = ()
    for n in range(len(counts)):
        result = (
            pl.pallas_call(
                functools.partial(kernel_b, plan, sum(counts[:n]), counts[n]),
                out_shape=vm((nv, blocks, width), F32),
                in_specs=[vmem_spec()] * (7 + len(result)),
                out_specs=vmem_spec(),
                scratch_shapes=[pltpu.VMEM((2 * width, 2 * width), BF)],
                input_output_aliases={7: 0} if result else {},
                compiler_params=params(12),
                name="local_part",
            )(fine_v, m1, mt1, mt2, lsm, sten_v, t_wide, *result),
        )

    done = [None] * ntop
    live = tops
    alive = list(range(ntop))
    message = msg
    halo_r = None
    for b in range(rounds):
        flip = (1 << b) | 1
        got = permute(message, lambda i: i ^ flip)
        if b == 0:
            halo_r = got[ntop]
            got = got[:ntop]
        live = live + got.astype(F32)
        keep = [p for p in range(len(alive)) if plan.spans[plan.top[alive[p]]] // blocks > 2 << b]
        for p in range(len(alive)):
            if p not in keep:
                done[alive[p]] = live[p]
        if keep and len(keep) < len(alive):
            live = live[keep[0] :]
        alive = [alive[p] for p in keep]
        message = live.astype(BF)
    sums = jnp.stack(done)

    per = 4
    slots = nv // per
    return pl.pallas_call(
        functools.partial(kernel_c, plan),
        out_shape=jax.ShapeDtypeStruct(fine.shape, F32),
        in_specs=[vmem_spec()] * 8,
        out_specs=any_spec(),
        scratch_shapes=[
            pltpu.VMEM((plan.top_cols * nv, width), F32),
            pltpu.VMEM((nv, width), F32),
            pltpu.VMEM((nv, width), F32),
            pltpu.VMEM((slots, per, blocks, width), F32),
            pltpu.SemaphoreType.DMA((slots,)),
        ],
        compiler_params=params(24),
        name="finish",
    )(*result, sums, halo_r, halo_o, mtop, sten_v, rt_top, inv_v)


def solution(mesh):
    in_specs = (P(None, "gx", None), P(None, "gx"), P(), P(), P())
    out_specs = P(None, "gx", None)

    return jax.shard_map(shards, mesh=mesh, in_specs=in_specs, out_specs=out_specs, check_vma=False)
```
